256 devices in a mesh: depth: 2 (over y_hi), row: 16 (over z, y_lo), col: 8 (over x, core).
Axes of the slice: x: 4, y: 4 (y_hi: 2, y_lo: 2; y = y_hi * 2 + y_lo), z: 8, core: 2. Of those that a mesh axis runs over, the one named last changes fastest.
Arguments:
- features: bfloat16 [128, 576, 1152], P('row', 'col', 'depth'), may hold values from -6 to 6
- w_in: bfloat16 [1152, 4096], P('depth'), may hold values from -0.1875 to 0.1875
- b_in: float32 [4096], replicated, may hold values from -4 to 4
- w_out: bfloat16 [4096, 4096], P('row', 'depth'), may hold values from -0.09375 to 0.09375
- b_out: float32 [4096], P('depth'), may hold values from -3 to 3
- text: bfloat16 [128, 448, 4096], P(('row', 'col'), None, 'depth'), may hold values from -6 to 6
- offsets: int32 [128], P(('row', 'col')), may hold values from 0 to 448
Outputs:
- sequences: bfloat16 [128, 1024, 4096], P(('row', 'col'), None, 'depth')
The draws below stay inside these ranges and needn't reach their ends.
Inputs may be any that keep to these rules, and one draw needn't show every extreme that they name: offsets[i] is where image i's first patch stands in sequence i.
All inputs are finite; a program needn't handle non-finite values.
Results may differ from the reference program's by a relative error of at most 0.007.
Values may be sent and summed in bfloat16 or wider, within the bound.
A program may use at most 128 MiB of HBM per device.

```python
import jax
import jax.numpy as jnp
from jax import lax

C = 1152
H = 4096
D = 4096
PATCHES = 576
TEXT = 448
IMAGES = 128


def set_ends(entries, own_key, least, largest):
    longest = entries.shape.index(max(entries.shape))
    spots = []
    for shift in (0, 1):
        where = [jax.random.randint(jax.random.fold_in(own_key, axis), (), 0, length) for axis, length in enumerate(entries.shape)]
        where[longest] = (where[longest] + shift) % entries.shape[longest]
        spots.append(tuple(where))
    return entries.at[spots[0]].set(least).at[spots[1]].set(largest)


def shard_levels(stream_key, extent, pieces, smallest, high):
    def one(position, blocks):
        heights = jax.random.uniform(jax.random.fold_in(jax.random.fold_in(stream_key, 6), position), (blocks,), jnp.float32, smallest / len(pieces), high / len(pieces))
        return jnp.repeat(jnp.exp(heights), extent[position] // blocks).reshape((-1,) + (1,) * (len(extent) - position - 1))

    gain = one(*pieces[0])
    for cut in pieces[1:]:
        gain = gain * one(*cut)
    return gain


def scatter_about(key, dims, scale, reach, pieces=(), held_as=jnp.bfloat16):
    drawn = scale * jax.random.normal(key, dims, jnp.float32)
    if pieces:
        drawn = drawn * shard_levels(key, dims, pieces, -0.22, 0.18)
    return jnp.clip(drawn, -reach, reach).astype(held_as)


def setup_inputs(seed: int = 0) -> dict:
    streams_of = jax.random.split(jax.random.key(seed), 8)
    return {
        "features": scatter_about(streams_of[0], (IMAGES, PATCHES, C), 1.0, 6.0, ((0, 16), (1, 8), (2, 2))),
        "w_in": scatter_about(streams_of[1], (C, H), C ** -0.5, 0.1875, ((0, 2),)),
        "b_in": scatter_about(streams_of[2], (H,), 1.0, 4.0, (), jnp.float32),
        "w_out": scatter_about(streams_of[3], (H, D), H ** -0.5, 0.09375, ((0, 16), (1, 2))),
        "b_out": scatter_about(streams_of[4], (D,), 0.5, 3.0, ((0, 2),), jnp.float32),
        "text": scatter_about(streams_of[5], (IMAGES, TEXT, D), 1.0, 6.0, ((0, 128), (2, 2))),
        "offsets": set_ends(jax.random.randint(streams_of[6], (IMAGES,), 0, TEXT + 1), jax.random.fold_in(streams_of[6], 1), 0, TEXT).astype(jnp.int32),
    }


def place_image(image_rows, text_rows, offset):
    patch_count = image_rows.shape[0]
    text_count = text_rows.shape[0]
    width = image_rows.shape[1]
    length = patch_count + text_count
    positions = jnp.arange(length, dtype=jnp.int32)
    zeros_text = jnp.zeros((text_count, width), image_rows.dtype)
    padded = jnp.concatenate([zeros_text, image_rows, zeros_text], 0)
    shifted = lax.dynamic_slice_in_dim(padded, (text_count - offset).astype(jnp.int32), length, 0)
    zeros_patch = jnp.zeros((patch_count, width), text_rows.dtype)
    early = jnp.concatenate([text_rows, zeros_patch], 0)
    later = jnp.concatenate([zeros_patch, text_rows], 0)
    inside = (positions >= offset) & (positions < offset + patch_count)
    before = positions < offset
    return jnp.where(inside[:, None], shifted, jnp.where(before[:, None], early, later))


def reference(features, w_in, b_in, w_out, b_out, text, offsets):
    half_width = C // 2

    def one_image(packed):
        image, text_rows, offset = packed
        first = jnp.dot(image[:, :half_width], w_in[:half_width], preferred_element_type=jnp.float32).astype(jnp.bfloat16)
        second = jnp.dot(image[:, half_width:], w_in[half_width:], preferred_element_type=jnp.float32).astype(jnp.bfloat16)
        first, second = lax.optimization_barrier((first, second))
        pre = first.astype(jnp.float32) + second.astype(jnp.float32) + b_in
        hidden = jax.nn.gelu(pre, approximate=False).astype(jnp.bfloat16)
        projected = (jnp.dot(hidden, w_out, preferred_element_type=jnp.float32) + b_out).astype(jnp.bfloat16)
        return place_image(projected, text_rows, offset)

    return lax.map(one_image, (features, text, offsets))
```

```python
import functools

import jax
import jax.numpy as jnp
from jax import lax
from jax.experimental import pallas as pl
from jax.experimental.pallas import tpu as pltpu
from jax.sharding import PartitionSpec as P

TILE = 16


def place_kernel(offset_ref, image_ref, text_ref, out_ref):
    offset = offset_ref[0]
    text_count = text_ref.shape[0]
    padded = image_ref.shape[0]
    patch_count = padded - TILE
    shift = lax.rem(offset, TILE)
    base = pl.multiple_of(offset - shift, TILE)
    out_ref[:text_count, :] = text_ref[...]
    out_ref[patch_count:, :] = text_ref[...]
    out_ref[pl.ds(pl.multiple_of(base + TILE, TILE), patch_count - TILE), :] = image_ref[TILE:patch_count, :]
    edge = pl.multiple_of(jnp.minimum(base, text_count - TILE), TILE)
    beside = text_ref[pl.ds(edge, TILE), :]
    rows = lax.broadcasted_iota(jnp.int32, beside.shape, 0)
    out_ref[pl.ds(base, TILE), :] = jnp.where(rows >= shift, image_ref[:TILE, :], beside)

    @pl.when(base < text_count)
    def _():
        below = jnp.where(rows < shift, image_ref[patch_count:, :], beside)
        out_ref[pl.ds(pl.multiple_of(base + patch_count, TILE), TILE), :] = below


def place(image_rows, text_rows, offset, width=512):
    padded, columns = image_rows.shape
    text_count = text_rows.shape[0]
    length = padded - TILE + text_count
    return pl.pallas_call(
        place_kernel,
        out_shape=jax.ShapeDtypeStruct((length, columns), image_rows.dtype),
        grid_spec=pltpu.PrefetchScalarGridSpec(
            num_scalar_prefetch=1,
            grid=(columns // width,),
            in_specs=[
                pl.BlockSpec((padded, width), lambda i, o: (0, i)),
                pl.BlockSpec((text_count, width), lambda i, o: (0, i)),
            ],
            out_specs=pl.BlockSpec((length, width), lambda i, o: (0, i)),
        ),
        name="place",
    )(offset, image_rows, text_rows)


def on_device(features, w_in, b_in, w_out, b_out, text, offsets):
    col = lax.axis_index("col")
    cols = lax.axis_size("col")
    image = lax.all_to_all(features, "col", split_axis=0, concat_axis=1, tiled=True)[0]
    image = lax.all_gather(image, "depth", axis=1, tiled=True)
    patch_count = image.shape[0]
    shift = lax.rem(offsets[0], TILE)
    spots = jnp.arange(patch_count + TILE, dtype=jnp.int32)[:, None] - shift
    moved = (spots == jnp.arange(patch_count, dtype=jnp.int32)[None, :]).astype(jnp.bfloat16)
    image = jnp.dot(moved, image, preferred_element_type=jnp.float32).astype(jnp.bfloat16)

    part = w_in.shape[0] // cols
    own_in = lax.dynamic_slice_in_dim(w_in, col * part, part, 0)
    full_in = lax.all_gather(own_in, ("depth", "col"), axis=0, tiled=True)
    pre = jnp.dot(image, full_in, preferred_element_type=jnp.float32) + b_in
    hidden = jax.nn.gelu(pre, approximate=False).astype(jnp.bfloat16)

    part = w_out.shape[0] // cols
    own_out = lax.dynamic_slice_in_dim(w_out, col * part, part, 0)
    full_out = lax.all_gather(own_out, ("row", "col"), axis=0, tiled=True)
    total = jnp.dot(hidden, full_out, preferred_element_type=jnp.float32)
    projected = (total + b_out).astype(jnp.bfloat16)
    return place(projected, text[0], offsets)[None]


def solution(mesh):
    return jax.shard_map(
        on_device,
        mesh=mesh,
        in_specs=(
            P("row", "col", "depth"),
            P("depth", None),
            P(),
            P("row", "depth"),
            P("depth"),
            P(("row", "col"), None, "depth"),
            P(("row", "col")),
        ),
        out_specs=P(("row", "col"), None, "depth"),
        check_vma=False,
    )
```

```python
import functools

import jax
import jax.numpy as jnp
from jax import lax
from jax.experimental import pallas as pl
from jax.experimental.pallas import tpu as pltpu
from jax.sharding import PartitionSpec as P

TILE = 16
MESH = pl.DeviceIdType.MESH
STEPS = 8
SLABS = 8
GROUP = 128


def place_kernel(offset_ref, image_ref, text_ref, out_ref):
    offset = offset_ref[0]
    text_count = text_ref.shape[0]
    padded = image_ref.shape[0]
    patch_count = padded - TILE
    shift = lax.rem(offset, TILE)
    base = pl.multiple_of(offset - shift, TILE)
    out_ref[:text_count, :] = text_ref[...]
    out_ref[patch_count:, :] = text_ref[...]
    out_ref[pl.ds(pl.multiple_of(base + TILE, TILE), patch_count - TILE), :] = image_ref[TILE:patch_count, :]
    edge = pl.multiple_of(jnp.minimum(base, text_count - TILE), TILE)
    beside = text_ref[pl.ds(edge, TILE), :]
    rows = lax.broadcasted_iota(jnp.int32, beside.shape, 0)
    out_ref[pl.ds(base, TILE), :] = jnp.where(rows >= shift, image_ref[:TILE, :], beside)

    @pl.when(base < text_count)
    def _():
        below = jnp.where(rows < shift, image_ref[patch_count:, :], beside)
        out_ref[pl.ds(pl.multiple_of(base + patch_count, TILE), TILE), :] = below


def place(image_rows, text_rows, offset, width=512):
    padded, columns = image_rows.shape
    text_count = text_rows.shape[0]
    length = padded - TILE + text_count
    return pl.pallas_call(
        place_kernel,
        out_shape=jax.ShapeDtypeStruct((length, columns), image_rows.dtype),
        grid_spec=pltpu.PrefetchScalarGridSpec(
            num_scalar_prefetch=1,
            grid=(columns // width,),
            in_specs=[
                pl.BlockSpec((padded, width), lambda i, o: (0, i)),
                pl.BlockSpec((text_count, width), lambda i, o: (0, i)),
            ],
            out_specs=pl.BlockSpec((length, width), lambda i, o: (0, i)),
        ),
        name="place",
    )(offset, image_rows, text_rows)


def project_kernel(
    shift_ref, features, w_in, b_in, w_out, b_out, out_ref,
    own_slabs, relay_slabs, far_slabs, tokens, own_image, far_image,
    own_in, far_in, pre, hidden, weights, total,
    local_sem, send_sem, recv_sem,
):
    depth, row, col = lax.axis_index("depth"), lax.axis_index("row"), lax.axis_index("col")
    z, low = lax.div(row, 2), lax.rem(row, 2)
    x, core = lax.div(col, 2), lax.rem(col, 2)
    twin = 2 * z + 1 - low
    beside = (depth, twin, col)
    across = (1 - depth, twin, col)
    up = (depth, 2 * lax.rem(z + 1, 8) + low, col)
    down = (depth, 2 * lax.rem(z + 7, 8) + low, col)
    ahead = (depth, row, 2 * lax.rem(x + 1, 4) + core)
    behind = (depth, row, 2 * lax.rem(x + 3, 4) + core)
    mate = (depth, row, 2 * x + 1 - core)

    def column(step, flip):
        return 2 * lax.rem(x + step, 4) + (1 - core if flip else core)

    def z_of(j):
        half, odd = lax.div(j + 1, 2), lax.rem(j, 2)
        return lax.rem(z + 8 + half * (1 - 2 * odd), 8)

    count = [0, 0]
    sent = []

    def local(source, target):
        copy = pltpu.make_async_copy(source, target, local_sem.at[count[0]])
        count[0] += 1
        copy.start()
        return copy

    def send(source, target, device):
        n = count[1]
        count[1] += 1
        copy = pltpu.make_async_remote_copy(
            src_ref=source, dst_ref=target, send_sem=send_sem.at[n], recv_sem=recv_sem.at[n],
            device_id=device, device_id_type=MESH,
        )
        copy.start()
        sent.append(copy)
        return copy

    def group_column(half, group):
        if group < 4:
            return 1024 * half + GROUP * group
        return 1024 * half + 512 + GROUP * lax.rem(x + group - 4, 4)

    own_weights = {}
    for near in (True, False):
        for group in range(8):
            half = core if near else 1 - core
            start = pl.multiple_of(group_column(half, group), GROUP)
            own_weights[near, group] = local(w_out.at[:, pl.ds(start, GROUP)], weights.at[row, half, group])
    own_slab = local(features.at[col], own_slabs.at[col])
    in_copies = []
    for j in range(STEPS):
        start = pl.multiple_of(512 * z_of(j), 512)
        in_copies.append(local(w_in.at[:, :, pl.ds(start, 512)], own_in.at[j]))

    others = [(0, True), (1, False), (1, True), (3, False), (3, True), (2, False), (2, True)]
    partners = [(depth, row, column(*other)) for other in others] + [beside, across, up, down]
    barrier = pltpu.get_barrier_semaphore()
    for partner in partners:
        pl.semaphore_signal(barrier, inc=1, device_id=partner, device_id_type=MESH)
    pl.semaphore_wait(barrier, len(partners))

    ring_up, ring_down, unit_mate, quarter, opposite, rest_mate = {}, {}, {}, {}, {}, {}

    def unit(b):
        return weights.at[b, core, pl.ds(0, 5)]

    def arrived_from(t, s, sign):
        return 2 * lax.rem(z + 8 + sign * t, 8) + (low if s == 0 else 1 - low)

    def onward(b, t, s, sign):
        ring = ring_up if sign < 0 else ring_down
        if t < 3 or (t == 3 and s == (0 if sign < 0 else 1)):
            ring[t, s] = send(unit(b), unit(b), up if sign < 0 else down)

    def spread(b, key):
        quarter[key] = (
            send(weights.at[b, core, 4], weights.at[b, core, 7], ahead),
            send(weights.at[b, core, 4], weights.at[b, core, 5], behind),
        )
        unit_mate[key] = send(unit(b), unit(b), mate)

    def block_of(key):
        t, s, sign = key
        return arrived_from(t, s, sign)

    def units(keys):
        for key in keys:
            t, s, sign = key
            (ring_up if sign < 0 else ring_down)[t - 1, s].wait_recv()
            onward(block_of(key), t, s, sign)
        for key in keys:
            spread(block_of(key), key)

    def quarters(keys):
        for key in keys:
            b = block_of(key)
            for copy in quarter[key]:
                copy.wait_recv()
            first, second = pl.ds(0, 128), pl.ds(128, 128)
            opposite[key] = (
                send(weights.at[b, core, 7, first], weights.at[b, core, 6, first], ahead),
                send(weights.at[b, core, 5, second], weights.at[b, core, 6, second], behind),
            )

    def opposites(keys):
        for key in keys:
            b = block_of(key)
            for copy in opposite[key]:
                copy.wait_recv()
            rest_mate[key] = send(weights.at[b, core, pl.ds(5, 3)], weights.at[b, core, pl.ds(5, 3)], mate)

    def complete(keys):
        for key in keys:
            unit_mate[key].wait_recv()
            rest_mate[key].wait_recv()

    for group in range(5):
        own_weights[True, group].wait()
    onward(row, 0, 0, -1)
    onward(row, 0, 0, 1)
    twin_unit = send(unit(row), unit(row), beside)
    slab_copies = {}
    for other in [others[1], others[2], others[3], others[4], others[5], others[6], others[0]]:
        target = column(*other)
        slab_copies[other] = send(features.at[target], own_slabs.at[col], (depth, row, target))

    mine, next_to = 2 * low + core, 2 * (1 - low) + core
    in_across, in_beside, in_mate, in_mate_next = {}, {}, {}, {}

    def in_start(j):
        in_copies[j].wait()
        in_across[j] = send(own_in.at[j, next_to], far_in.at[j, next_to], across)

    def in_pass(j):
        in_across[j].wait_recv()
        in_beside[j] = send(far_in.at[j, mine], far_in.at[j, mine], beside)
        in_mate[j] = send(far_in.at[j, mine], far_in.at[j, mine], mate)

    def in_pass_next(j):
        in_beside[j].wait_recv()
        in_mate_next[j] = send(far_in.at[j, next_to], far_in.at[j, next_to], mate)

    def in_complete(j):
        in_mate[j].wait_recv()
        in_mate_next[j].wait_recv()

    in_start(0)
    in_start(1)

    hops, lasts, slab_at = [], [], []

    def hop(slab):
        n = len(hops)
        slab_at.append(slab)
        hops.append(send(own_slabs.at[slab], relay_slabs.at[slab], beside if n % 2 == 0 else across))

    def relay(n):
        hops[n].wait_recv()
        slab = slab_at[n]
        lasts.append(send(relay_slabs.at[slab], far_slabs.at[slab], across if n % 2 == 0 else beside))

    def source_of(other):
        step, flip = other
        return column((4 - step) % 4, flip)

    def take(other):
        slab_copies[other].wait_recv()
        hop(source_of(other))

    own_slab.wait()
    hop(col)
    for other in (others[0], others[1], others[2], others[3], others[4]):
        take(other)
    relay(0)
    relay(1)
    twin_unit.wait_recv()
    twin_key = (0, 1, 1)
    onward(twin, 0, 1, -1)
    onward(twin, 0, 1, 1)
    spread(twin, twin_key)
    take(others[5])
    take(others[6])
    for n in range(2, 6):
        relay(n)

    patch_count = tokens.shape[0]
    spots = lax.broadcasted_iota(jnp.int32, (patch_count + TILE, patch_count), 0) - shift_ref[0]
    moved = (spots == lax.broadcasted_iota(jnp.int32, spots.shape, 1)).astype(jnp.float32).astype(jnp.bfloat16)

    def assemble(slabs, image):
        height = slabs.shape[1]
        for slab in range(SLABS):
            tokens[slab * height : (slab + 1) * height, :] = slabs[slab].astype(jnp.float32)
        image[...] = jnp.dot(
            moved, tokens[...].astype(jnp.bfloat16), preferred_element_type=jnp.float32
        ).astype(jnp.bfloat16)

    def half_columns(n):
        return pl.ds(pl.multiple_of(256 * n, 256), 256)

    def own_layer(first, last):
        def body(i, carry):
            j, n = lax.div(i, 2), lax.rem(i, 2)
            rhs = own_in[j, :, :, half_columns(n)].reshape(-1, 256)
            pre[j, :, half_columns(n)] = jnp.dot(own_image[...], rhs, preferred_element_type=jnp.float32)
            return carry

        lax.fori_loop(2 * first, 2 * last, body, 0)

    def first_layer(first, last):
        def body(i, carry):
            j, n = lax.div(i, 2), lax.rem(i, 2)
            rhs = far_in[j, :, :, half_columns(n)].reshape(-1, 256)
            value = pre[j, :, half_columns(n)] + jnp.dot(far_image[...], rhs, preferred_element_type=jnp.float32)
            value = value + b_in[pl.ds(z_of(j), 1), half_columns(n)]
            value = 0.5 * value * (1.0 + lax.erf(value * 0.7071067811865476))
            hidden[j, :, half_columns(n)] = value.astype(jnp.bfloat16)
            return carry

        lax.fori_loop(2 * first, 2 * last, body, 0)

    def product(j, n):
        half, group = lax.div(n, 4), 2 * lax.rem(n, 4)
        b = 2 * z_of(j)
        rhs = jnp.concatenate(
            [
                jnp.concatenate([weights[b + s, half, group], weights[b + s, half, group + 1]], axis=1)
                for s in range(2)
            ],
            axis=0,
        )
        return jnp.dot(hidden[j], rhs, preferred_element_type=jnp.float32)

    def second_layer(first, last):
        def body(i, carry):
            j, n = first + lax.div(i, 8), lax.rem(i, 8)
            if first == 0:
                total[n] = product(j, n)
            else:
                total[n] += product(j, n)
            return carry

        lax.fori_loop(0, 8 * (last - first), body, 0)

    near1 = [(1, 0, -1), (1, 0, 1)]
    units(near1)
    assemble(own_slabs, own_image)
    relay(6)
    relay(7)
    for j in range(2, STEPS):
        in_start(j)
    quarters([twin_key])
    in_pass(0)
    in_pass(1)
    own_layer(0, 3)
    opposites([twin_key])
    quarters(near1)
    own_layer(3, 5)
    opposites(near1)
    in_pass_next(0)
    in_pass_next(1)
    far1 = [(1, 1, -1), (1, 1, 1)]
    units(far1)
    own_layer(5, 8)
    for last in lasts:
        last.wait_recv()
    quarters(far1)
    assemble(far_slabs, far_image)
    in_complete(0)
    in_complete(1)
    opposites(far1)
    in_pass(2)
    first_layer(0, 1)
    for (near, group), copy in own_weights.items():
        if not near or group >= 5:
            copy.wait()
    complete([twin_key])
    second_layer(0, 1)

    near2 = [(2, 0, -1), (2, 0, 1)]
    units(near2)
    in_pass_next(2)
    in_pass(3)
    first_layer(1, 2)
    quarters(near2)
    in_pass_next(3)
    in_complete(2)
    first_layer(2, 3)
    opposites(near2)
    in_pass(4)
    complete(near1)
    complete(far1)
    second_layer(1, 3)

    far2 = [(2, 1, -1), (2, 1, 1)]
    units(far2)
    in_pass_next(4)
    in_pass(5)
    in_complete(3)
    first_layer(3, 4)
    quarters(far2)
    in_pass_next(5)
    in_complete(4)
    first_layer(4, 5)
    opposites(far2)
    in_pass(6)

    near3 = [(3, 0, -1), (3, 0, 1)]
    units(near3)
    complete(near2)
    complete(far2)
    second_layer(3, 5)
    in_pass_next(6)
    in_pass(7)
    quarters(near3)
    in_complete(5)
    first_layer(5, 6)
    in_pass_next(7)
    in_complete(6)
    opposites(near3)
    first_layer(6, 7)
    in_complete(7)
    first_layer(7, 8)

    far3 = [(3, 1, -1), (3, 1, 1)]
    units(far3)
    quarters(far3)
    opposites(far3)
    complete(near3)
    complete(far3)
    second_layer(5, 7)

    final = [(4, 0, -1), (4, 1, 1)]
    units(final)
    quarters(final)
    opposites(final)
    complete(final)

    def finish(n, carry):
        half, group = lax.div(n, 4), 2 * lax.rem(n, 4)
        value = total[n] + product(7, n)
        for side in range(2):
            g = group + side
            turned = lax.rem(x + g, 4)
            in_first = lax.div(4 + 3 - g, 4)
            place_at = in_first * g + (1 - in_first) * (4 + turned)
            start = pl.multiple_of(1024 * half + GROUP * place_at, GROUP)
            part = value[:, side * GROUP : (side + 1) * GROUP] + b_out[:, pl.ds(start, GROUP)]
            out_ref[:, pl.ds(start, GROUP)] = part.astype(jnp.bfloat16)
        return carry

    lax.fori_loop(0, 8, finish, 0)
    for copy in sent:
        copy.wait_send()


LOCALS = 25
SENDS = 160


def project(shift, features, w_in, b_in, w_out, b_out):
    slabs, height, width = features.shape
    tokens = slabs * height
    padded = tokens + TILE
    hidden = w_in.shape[1]
    columns = w_out.shape[1]
    block = w_out.shape[0]
    chunk = hidden // STEPS
    bf16, f32 = jnp.bfloat16, jnp.float32
    anywhere = pl.BlockSpec(memory_space=pl.ANY)
    vmem = pl.BlockSpec(memory_space=pltpu.VMEM)
    quarter = width // 4
    flops = 2 * padded * (2 * width * hidden + hidden * columns)
    return pl.pallas_call(
        project_kernel,
        out_shape=jax.ShapeDtypeStruct((padded, columns), bf16),
        in_specs=[pl.BlockSpec(memory_space=pltpu.SMEM), anywhere, anywhere, vmem, anywhere, vmem],
        out_specs=vmem,
        scratch_shapes=[
            pltpu.VMEM((slabs, height, width), bf16),
            pltpu.VMEM((slabs, height, width), bf16),
            pltpu.VMEM((slabs, height, width), bf16),
            pltpu.VMEM((tokens, width), f32),
            pltpu.VMEM((padded, width), bf16),
            pltpu.VMEM((padded, width), bf16),
            pltpu.VMEM((STEPS, 4, quarter, chunk), bf16),
            pltpu.VMEM((STEPS, 4, quarter, chunk), bf16),
            pltpu.VMEM((STEPS, padded, chunk), f32),
            pltpu.VMEM((STEPS, padded, chunk), bf16),
            pltpu.VMEM((16, 2, 8, block, GROUP), bf16),
            pltpu.VMEM((8, padded, 2 * GROUP), f32),
            pltpu.SemaphoreType.DMA((LOCALS,)),
            pltpu.SemaphoreType.DMA((SENDS,)),
            pltpu.SemaphoreType.DMA((SENDS,)),
        ],
        compiler_params=pltpu.CompilerParams(
            collective_id=0, has_side_effects=True, vmem_limit_bytes=67_043_328
        ),
        cost_estimate=pl.CostEstimate(flops=flops, bytes_accessed=10_000_000, transcendentals=padded * hidden),
        name="project",
    )(shift, features, w_in.reshape(4, quarter, hidden), b_in.reshape(STEPS, chunk), w_out, b_out.reshape(1, columns))


def on_device(features, w_in, b_in, w_out, b_out, text, offsets):
    shift = lax.rem(offsets, TILE)
    projected = project(shift, features, w_in, b_in, w_out, b_out)
    return place(projected, text[0], offsets)[None]


def solution(mesh):
    return jax.shard_map(
        on_device,
        mesh=mesh,
        in_specs=(
            P("row", "col", "depth"),
            P("depth", None),
            P(),
            P("row", "depth"),
            P("depth"),
            P(("row", "col"), None, "depth"),
            P(("row", "col")),
        ),
        out_specs=P(("row", "col"), None, "depth"),
        check_vma=False,
    )
```

```python
import functools

import jax
import jax.numpy as jnp
from jax import lax
from jax.experimental import pallas as pl
from jax.experimental.pallas import tpu as pltpu
from jax.sharding import PartitionSpec as P

TILE = 16
MESH = pl.DeviceIdType.MESH
STEPS = 8
SLABS = 8
GROUP = 128


def place_kernel(offset_ref, image_ref, text_ref, out_ref):
    offset = offset_ref[0]
    text_count = text_ref.shape[0]
    padded = image_ref.shape[0]
    patch_count = padded - TILE
    shift = lax.rem(offset, TILE)
    base = pl.multiple_of(offset - shift, TILE)
    out_ref[:text_count, :] = text_ref[...]
    out_ref[patch_count:, :] = text_ref[...]
    out_ref[pl.ds(pl.multiple_of(base + TILE, TILE), patch_count - TILE), :] = image_ref[TILE:patch_count, :]
    edge = pl.multiple_of(jnp.minimum(base, text_count - TILE), TILE)
    beside = text_ref[pl.ds(edge, TILE), :]
    rows = lax.broadcasted_iota(jnp.int32, beside.shape, 0)
    out_ref[pl.ds(base, TILE), :] = jnp.where(rows >= shift, image_ref[:TILE, :], beside)

    @pl.when(base < text_count)
    def _():
        below = jnp.where(rows < shift, image_ref[patch_count:, :], beside)
        out_ref[pl.ds(pl.multiple_of(base + patch_count, TILE), TILE), :] = below


def place(image_rows, text_rows, offset, width=512):
    padded, columns = image_rows.shape
    text_count = text_rows.shape[0]
    length = padded - TILE + text_count
    return pl.pallas_call(
        place_kernel,
        out_shape=jax.ShapeDtypeStruct((length, columns), image_rows.dtype),
        grid_spec=pltpu.PrefetchScalarGridSpec(
            num_scalar_prefetch=1,
            grid=(columns // width,),
            in_specs=[
                pl.BlockSpec((padded, width), lambda i, o: (0, i)),
                pl.BlockSpec((text_count, width), lambda i, o: (0, i)),
            ],
            out_specs=pl.BlockSpec((length, width), lambda i, o: (0, i)),
        ),
        name="place",
    )(offset, image_rows, text_rows)


def project_kernel(
    shift_ref, features, w_in, b_in, w_out, b_out, out_ref,
    own_slabs, relay_slabs, far_slabs, tokens, own_image, far_image,
    own_in, far_in, pre, hidden, weights, total,
    local_sem, send_sem, recv_sem,
):
    depth, row, col = lax.axis_index("depth"), lax.axis_index("row"), lax.axis_index("col")
    z, low = lax.div(row, 2), lax.rem(row, 2)
    x, core = lax.div(col, 2), lax.rem(col, 2)
    twin = 2 * z + 1 - low
    beside = (depth, twin, col)
    across = (1 - depth, twin, col)
    up = (depth, 2 * lax.rem(z + 1, 8) + low, col)
    down = (depth, 2 * lax.rem(z + 7, 8) + low, col)
    ahead = (depth, row, 2 * lax.rem(x + 1, 4) + core)
    behind = (depth, row, 2 * lax.rem(x + 3, 4) + core)
    mate = (depth, row, 2 * x + 1 - core)

    def column(step, flip):
        return 2 * lax.rem(x + step, 4) + (1 - core if flip else core)

    def z_of(j):
        half, odd = lax.div(j + 1, 2), lax.rem(j, 2)
        return lax.rem(z + 8 + half * (1 - 2 * odd), 8)

    count = [0, 0]
    sent = []

    def local(source, target):
        copy = pltpu.make_async_copy(source, target, local_sem.at[count[0]])
        count[0] += 1
        copy.start()
        return copy

    def send(source, target, device):
        n = count[1]
        count[1] += 1
        copy = pltpu.make_async_remote_copy(
            src_ref=source, dst_ref=target, send_sem=send_sem.at[n], recv_sem=recv_sem.at[n],
            device_id=device, device_id_type=MESH,
        )
        copy.start()
        sent.append(copy)
        return copy

    def group_column(half, group):
        if group < 4:
            return 1024 * half + GROUP * group
        return 1024 * half + 512 + GROUP * lax.rem(x + group - 4, 4)

    own_weights = {}
    for near in (True, False):
        for group in range(8):
            half = core if near else 1 - core
            start = pl.multiple_of(group_column(half, group), GROUP)
            own_weights[near, group] = local(w_out.at[:, pl.ds(start, GROUP)], weights.at[row, half, group])
    own_slab = local(features.at[col], own_slabs.at[col])
    in_copies = []
    for j in range(STEPS):
        start = pl.multiple_of(512 * z_of(j), 512)
        in_copies.append(local(w_in.at[:, :, pl.ds(start, 512)], own_in.at[j]))

    others = [(0, True), (1, False), (1, True), (3, False), (3, True), (2, False), (2, True)]
    partners = [(depth, row, column(*other)) for other in others] + [beside, across, up, down]
    barrier = pltpu.get_barrier_semaphore()
    for partner in partners:
        pl.semaphore_signal(barrier, inc=1, device_id=partner, device_id_type=MESH)
    pl.semaphore_wait(barrier, len(partners))

    ring, quarter, opposite, first_mate, second_mate = {}, {}, {}, {}, {}

    def columns_of(b, part):
        return weights.at[b, core, pl.ds(0, 4)] if part == "first" else weights.at[b, core, 4]

    def block_of(key):
        t, s, sign = key
        return 2 * lax.rem(z + 8 + sign * t, 8) + (low if s == 0 else 1 - low)

    def onward(key, part):
        t, s, sign = key
        if t < 3 or (t == 3 and s == (0 if sign < 0 else 1)):
            b = block_of(key)
            ring[key, part] = send(columns_of(b, part), columns_of(b, part), up if sign < 0 else down)

    def came(key, part):
        t, s, sign = key
        ring[(t - 1, s, sign), part].wait_recv()

    def spread(key):
        b = block_of(key)
        quarter[key] = (
            send(weights.at[b, core, 4], weights.at[b, core, 7], ahead),
            send(weights.at[b, core, 4], weights.at[b, core, 5], behind),
        )

    def pass_first(key):
        b = block_of(key)
        first_mate[key] = send(columns_of(b, "first"), columns_of(b, "first"), mate)

    def firsts(keys):
        for key in keys:
            came(key, "first")
            onward(key, "first")
        for key in keys:
            pass_first(key)

    def seconds(keys):
        for key in keys:
            came(key, "second")
            onward(key, "second")

    def spreads(keys):
        for key in keys:
            spread(key)

    def quarters(keys):
        for key in keys:
            b = block_of(key)
            for copy in quarter[key]:
                copy.wait_recv()
            above, below = pl.ds(0, 128), pl.ds(128, 128)
            opposite[key] = (
                send(weights.at[b, core, 7, above], weights.at[b, core, 6, above], ahead),
                send(weights.at[b, core, 5, below], weights.at[b, core, 6, below], behind),
            )

    def opposites(keys):
        for key in keys:
            b = block_of(key)
            for copy in opposite[key]:
                copy.wait_recv()
            second_mate[key] = send(weights.at[b, core, pl.ds(4, 4)], weights.at[b, core, pl.ds(4, 4)], mate)

    def complete(keys):
        for key in keys:
            first_mate[key].wait_recv()
            second_mate[key].wait_recv()

    def twin_seconds():
        twin_second.wait_recv()
        onward((0, 1, -1), "second")
        onward((0, 1, 1), "second")

    def twin_firsts():
        twin_first.wait_recv()
        onward((0, 1, -1), "first")
        onward((0, 1, 1), "first")
        pass_first((0, 1, 1))

    own_weights[True, 4].wait()
    onward((0, 0, -1), "second")
    onward((0, 0, 1), "second")
    twin_second = send(columns_of(row, "second"), columns_of(row, "second"), beside)
    for group in range(4):
        own_weights[True, group].wait()
    onward((0, 0, -1), "first")
    onward((0, 0, 1), "first")
    twin_first = send(columns_of(row, "first"), columns_of(row, "first"), beside)
    slab_copies = {}
    for other in [others[1], others[2], others[3], others[4], others[5], others[6], others[0]]:
        target = column(*other)
        slab_copies[other] = send(features.at[target], own_slabs.at[col], (depth, row, target))

    mine, next_to = 2 * low + core, 2 * (1 - low) + core
    in_across, in_beside, in_mate, in_mate_next = {}, {}, {}, {}

    def in_start(j):
        in_copies[j].wait()
        in_across[j] = send(own_in.at[j, next_to], far_in.at[j, next_to], across)

    def in_pass(j):
        in_across[j].wait_recv()
        in_beside[j] = send(far_in.at[j, mine], far_in.at[j, mine], beside)
        in_mate[j] = send(far_in.at[j, mine], far_in.at[j, mine], mate)

    def in_pass_next(j):
        in_beside[j].wait_recv()
        in_mate_next[j] = send(far_in.at[j, next_to], far_in.at[j, next_to], mate)

    def in_complete(j):
        in_mate[j].wait_recv()
        in_mate_next[j].wait_recv()


    hops, lasts, slab_at = {}, {}, {}

    def hop(n, slab):
        slab_at[n] = slab
        hops[n] = send(own_slabs.at[slab], relay_slabs.at[slab], beside if n % 2 == 0 else across)

    def relay(n):
        hops[n].wait_recv()
        slab = slab_at[n]
        lasts[n] = send(relay_slabs.at[slab], far_slabs.at[slab], across if n % 2 == 0 else beside)

    def source_of(other):
        step, flip = other
        return column((4 - step) % 4, flip)

    def take(n):
        if n == 0:
            own_slab.wait()
            hop(0, col)
        else:
            slab_copies[others[n - 1]].wait_recv()
            hop(n, source_of(others[n - 1]))

    patch_count = tokens.shape[0]
    spots = lax.broadcasted_iota(jnp.int32, (patch_count + TILE, patch_count), 0) - shift_ref[0]
    moved = (spots == lax.broadcasted_iota(jnp.int32, spots.shape, 1)).astype(jnp.float32).astype(jnp.bfloat16)

    def assemble(slabs, image):
        height = slabs.shape[1]
        for slab in range(SLABS):
            tokens[slab * height : (slab + 1) * height, :] = slabs[slab].astype(jnp.float32)
        image[...] = jnp.dot(
            moved, tokens[...].astype(jnp.bfloat16), preferred_element_type=jnp.float32
        ).astype(jnp.bfloat16)

    def half_columns(n):
        return pl.ds(pl.multiple_of(256 * n, 256), 256)

    def own_layer(first, last):
        def body(i, carry):
            j, n = lax.div(i, 2), lax.rem(i, 2)
            rhs = own_in[j, :, :, half_columns(n)].reshape(-1, 256)
            pre[j, :, half_columns(n)] = jnp.dot(own_image[...], rhs, preferred_element_type=jnp.float32)
            return carry

        lax.fori_loop(2 * first, 2 * last, body, 0)

    def first_layer(first, last):
        def body(i, carry):
            j, n = lax.div(i, 2), lax.rem(i, 2)
            rhs = far_in[j, :, :, half_columns(n)].reshape(-1, 256)
            value = pre[j, :, half_columns(n)] + jnp.dot(far_image[...], rhs, preferred_element_type=jnp.float32)
            value = value + b_in[:, pl.ds(pl.multiple_of(512 * z_of(j) + 256 * n, 256), 256)]
            value = 0.5 * value * (1.0 + lax.erf(value * 0.7071067811865476))
            hidden[j, :, half_columns(n)] = value.astype(jnp.bfloat16)
            return carry

        lax.fori_loop(2 * first, 2 * last, body, 0)

    def product(j, half, group):
        b = 2 * z_of(j)
        rhs = jnp.concatenate(
            [
                jnp.concatenate([weights[b + s, half, group], weights[b + s, half, group + 1]], axis=1)
                for s in range(2)
            ],
            axis=0,
        )
        return jnp.dot(hidden[j], rhs, preferred_element_type=jnp.float32)

    def second_layer(first, last):
        def body(i, carry):
            j, half = first + lax.div(i, 2), lax.rem(i, 2)
            for pair in range(4):
                n = 4 * half + pair
                if first == 0:
                    total[n] = product(j, half, 2 * pair)
                else:
                    total[n] += product(j, half, 2 * pair)
            return carry

        lax.fori_loop(0, 2 * (last - first), body, 0)

    in_start(0)
    take(0)
    in_start(1)
    seconds([(1, 0, 1)])
    seconds([(1, 0, -1)])
    in_start(2)
    in_start(3)
    in_pass(0)
    twin_seconds()
    spreads([(1, 0, -1)])
    spreads([(0, 1, 1)])
    twin_firsts()
    take(2)
    seconds([(1, 1, 1)])
    take(6)
    take(3)
    take(1)
    seconds([(1, 1, -1)])
    seconds([(2, 0, 1)])
    spreads([(2, 0, 1)])
    spreads([(1, 1, -1)])
    in_pass(2)
    quarters([(0, 1, 1)])
    seconds([(2, 0, -1)])
    take(7)
    take(4)
    take(5)
    assemble(own_slabs, own_image)
    spreads([(1, 1, 1)])
    firsts([(1, 0, -1)])
    relay(3)
    spreads([(2, 0, -1)])
    firsts([(1, 1, 1)])
    relay(2)
    seconds([(2, 1, -1)])
    spreads([(2, 1, -1)])
    relay(0)
    opposites([(0, 1, 1)])
    own_layer(0, 1)
    seconds([(2, 1, 1)])
    spreads([(2, 1, 1)])
    in_start(4)
    in_pass(1)
    firsts([(1, 0, 1)])
    firsts([(1, 1, -1)])
    seconds([(3, 0, 1)])
    quarters([(2, 0, 1)])
    relay(5)
    relay(6)
    relay(4)
    quarters([(1, 0, -1)])
    quarters([(2, 0, -1)])
    in_start(5)
    own_layer(1, 2)
    relay(7)
    relay(1)
    seconds([(3, 0, -1)])
    spreads([(3, 0, 1)])
    quarters([(1, 1, 1)])
    own_layer(2, 3)
    in_start(6)
    quarters([(2, 1, -1)])
    spreads([(3, 0, -1)])
    own_layer(3, 6)
    in_pass_next(0)
    in_start(7)
    quarters([(1, 1, -1)])
    seconds([(3, 1, -1)])
    quarters([(2, 1, 1)])
    opposites([(2, 0, -1)])
    in_pass_next(2)
    opposites([(1, 0, -1)])
    firsts([(2, 0, -1)])
    in_pass(3)
    in_pass_next(1)
    seconds([(3, 1, 1)])
    spreads([(3, 1, -1)])
    in_pass(4)
    spreads([(3, 1, 1)])
    firsts([(2, 1, 1)])
    spreads([(1, 0, 1)])
    own_layer(6, 7)
    opposites([(2, 1, -1)])
    own_layer(7, 8)
    for last in lasts.values():
        last.wait_recv()
    assemble(far_slabs, far_image)
    opposites([(1, 1, 1)])
    in_complete(0)
    first_layer(0, 1)
    firsts([(2, 0, 1)])
    quarters([(3, 1, -1)])
    in_complete(2)
    first_layer(2, 3)
    firsts([(2, 1, -1)])
    seconds([(4, 1, 1)])
    quarters([(3, 0, 1)])
    in_pass_next(3)
    spreads([(4, 1, 1)])
    seconds([(4, 0, -1)])
    in_pass(5)
    for (near, group), copy in own_weights.items():
        if not near or group >= 5:
            copy.wait()
    complete([(0, 1, 1)])
    second_layer(0, 1)
    quarters([(3, 1, 1)])
    spreads([(4, 0, -1)])
    in_complete(1)
    first_layer(1, 2)
    quarters([(1, 0, 1)])
    in_pass(6)
    opposites([(1, 1, -1)])
    in_pass_next(4)
    quarters([(3, 0, -1)])
    opposites([(2, 1, 1)])
    in_complete(3)
    first_layer(3, 4)
    opposites([(2, 0, 1)])
    complete([(2, 0, -1), (2, 1, -1)])
    second_layer(3, 4)
    in_complete(4)
    first_layer(4, 5)
    in_pass_next(5)
    firsts([(3, 1, 1)])
    firsts([(3, 0, -1)])
    opposites([(3, 1, -1)])
    quarters([(4, 1, 1)])
    in_pass(7)
    complete([(2, 0, 1), (2, 1, 1)])
    second_layer(4, 5)
    opposites([(3, 1, 1)])
    in_complete(5)
    first_layer(5, 6)
    in_pass_next(6)
    opposites([(3, 0, 1)])
    quarters([(4, 0, -1)])
    firsts([(3, 0, 1)])
    opposites([(3, 0, -1)])
    opposites([(1, 0, 1)])
    complete([(1, 0, -1), (1, 1, -1)])
    second_layer(1, 2)
    firsts([(3, 1, -1)])
    in_complete(6)
    first_layer(6, 7)
    complete([(3, 0, 1), (3, 1, 1)])
    second_layer(6, 7)
    opposites([(4, 0, -1)])
    in_pass_next(7)
    opposites([(4, 1, 1)])
    complete([(3, 0, -1), (3, 1, -1)])
    second_layer(5, 6)
    firsts([(4, 1, 1)])
    firsts([(4, 0, -1)])
    complete([(1, 0, 1), (1, 1, 1)])
    second_layer(2, 3)
    in_complete(7)
    first_layer(7, 8)
    complete([(4, 0, -1), (4, 1, 1)])

    def finish(half, carry):
        for pair in range(4):
            value = total[4 * half + pair] + product(7, half, 2 * pair)
            for side in range(2):
                group = 2 * pair + side
                start = pl.multiple_of(group_column(half, group), GROUP)
                part = value[:, side * GROUP : (side + 1) * GROUP] + b_out[:, pl.ds(start, GROUP)]
                out_ref[:, pl.ds(start, GROUP)] = part.astype(jnp.bfloat16)
        return carry

    lax.fori_loop(0, 2, finish, 0)
    for copy in sent:
        copy.wait_send()


LOCALS = 25
SENDS = 175


def project(shift, features, w_in, b_in, w_out, b_out):
    slabs, height, width = features.shape
    tokens = slabs * height
    padded = tokens + TILE
    hidden = w_in.shape[1]
    columns = w_out.shape[1]
    block = w_out.shape[0]
    chunk = hidden // STEPS
    bf16, f32 = jnp.bfloat16, jnp.float32
    anywhere = pl.BlockSpec(memory_space=pltpu.HBM)
    vmem = pl.BlockSpec(memory_space=pltpu.VMEM)
    quarter = width // 4
    flops = 2 * padded * (2 * width * hidden + hidden * columns)
    return pl.pallas_call(
        project_kernel,
        out_shape=jax.ShapeDtypeStruct((padded, columns), bf16),
        in_specs=[pl.BlockSpec(memory_space=pltpu.SMEM), anywhere, anywhere, vmem, anywhere, vmem],
        out_specs=vmem,
        scratch_shapes=[
            pltpu.VMEM((slabs, height, width), bf16),
            pltpu.VMEM((slabs, height, width), bf16),
            pltpu.VMEM((slabs, height, width), bf16),
            pltpu.VMEM((tokens, width), f32),
            pltpu.VMEM((padded, width), bf16),
            pltpu.VMEM((padded, width), bf16),
            pltpu.VMEM((STEPS, 4, quarter, chunk), bf16),
            pltpu.VMEM((STEPS, 4, quarter, chunk), bf16),
            pltpu.VMEM((STEPS, padded, chunk), f32),
            pltpu.VMEM((STEPS, padded, chunk), bf16),
            pltpu.VMEM((16, 2, 8, block, GROUP), bf16),
            pltpu.VMEM((8, padded, 2 * GROUP), f32),
            pltpu.SemaphoreType.DMA((LOCALS,)),
            pltpu.SemaphoreType.DMA((SENDS,)),
            pltpu.SemaphoreType.DMA((SENDS,)),
        ],
        compiler_params=pltpu.CompilerParams(
            collective_id=0, has_side_effects=True, vmem_limit_bytes=58_000_000
        ),
        cost_estimate=pl.CostEstimate(flops=flops, bytes_accessed=10_000_000, transcendentals=padded * hidden),
        name="project",
    )(shift, features, w_in.reshape(4, quarter, hidden), b_in.reshape(1, hidden), w_out, b_out.reshape(1, columns))


def on_device(features, w_in, b_in, w_out, b_out, text, offsets):
    shift = lax.rem(offsets, TILE)
    projected = project(shift, features, w_in, b_in, w_out, b_out)
    return place(projected, text[0], offsets)[None]


def solution(mesh):
    return jax.shard_map(
        on_device,
        mesh=mesh,
        in_specs=(
            P("row", "col", "depth"),
            P("depth", None),
            P(),
            P("row", "depth"),
            P("depth"),
            P(("row", "col"), None, "depth"),
            P(("row", "col")),
        ),
        out_specs=P(("row", "col"), None, "depth"),
        check_vma=False,
    )
```

```python
import functools

import jax
import jax.numpy as jnp
from jax import lax
from jax.experimental import pallas as pl
from jax.experimental.pallas import tpu as pltpu
from jax.sharding import PartitionSpec as P

TILE = 16
MESH = pl.DeviceIdType.MESH
STEPS = 8
SLABS = 8
GROUP = 128


def place_kernel(offset_ref, image_ref, text_ref, out_ref):
    offset = offset_ref[0]
    text_count = text_ref.shape[0]
    padded = image_ref.shape[0]
    patch_count = padded - TILE
    shift = lax.rem(offset, TILE)
    base = pl.multiple_of(offset - shift, TILE)
    out_ref[:text_count, :] = text_ref[...]
    out_ref[patch_count:, :] = text_ref[...]
    out_ref[pl.ds(pl.multiple_of(base + TILE, TILE), patch_count - TILE), :] = image_ref[TILE:patch_count, :]
    edge = pl.multiple_of(jnp.minimum(base, text_count - TILE), TILE)
    beside = text_ref[pl.ds(edge, TILE), :]
    rows = lax.broadcasted_iota(jnp.int32, beside.shape, 0)
    out_ref[pl.ds(base, TILE), :] = jnp.where(rows >= shift, image_ref[:TILE, :], beside)

    @pl.when(base < text_count)
    def _():
        below = jnp.where(rows < shift, image_ref[patch_count:, :], beside)
        out_ref[pl.ds(pl.multiple_of(base + patch_count, TILE), TILE), :] = below


def place(image_rows, text_rows, offset, width=1024):
    padded, columns = image_rows.shape
    text_count = text_rows.shape[0]
    length = padded - TILE + text_count
    return pl.pallas_call(
        place_kernel,
        out_shape=jax.ShapeDtypeStruct((length, columns), image_rows.dtype),
        grid_spec=pltpu.PrefetchScalarGridSpec(
            num_scalar_prefetch=1,
            grid=(columns // width,),
            in_specs=[
                pl.BlockSpec((padded, width), lambda i, o: (0, i)),
                pl.BlockSpec((text_count, width), lambda i, o: (0, i)),
            ],
            out_specs=pl.BlockSpec((length, width), lambda i, o: (0, i)),
        ),
        name="place",
    )(offset, image_rows, text_rows)


def project_kernel(
    shift_ref, features, w_in, b_in, w_out, b_out, out_ref,
    own_slabs, relay_slabs, far_slabs, tokens, own_image, far_image,
    own_in, far_in, pre, hidden, weights, total, out_rows,
    local_sem, send_sem, recv_sem,
):
    depth, row, col = lax.axis_index("depth"), lax.axis_index("row"), lax.axis_index("col")
    z, low = lax.div(row, 2), lax.rem(row, 2)
    x, core = lax.div(col, 2), lax.rem(col, 2)
    twin = 2 * z + 1 - low
    beside = (depth, twin, col)
    across = (1 - depth, twin, col)
    up = (depth, 2 * lax.rem(z + 1, 8) + low, col)
    down = (depth, 2 * lax.rem(z + 7, 8) + low, col)
    ahead = (depth, row, 2 * lax.rem(x + 1, 4) + core)
    behind = (depth, row, 2 * lax.rem(x + 3, 4) + core)
    mate = (depth, row, 2 * x + 1 - core)

    def column(step, flip):
        return 2 * lax.rem(x + step, 4) + (1 - core if flip else core)

    def z_of(j):
        half, odd = lax.div(j + 1, 2), lax.rem(j, 2)
        return lax.rem(z + 8 + half * (1 - 2 * odd), 8)

    count = [0, 0]
    sent = []

    def local(source, target):
        copy = pltpu.make_async_copy(source, target, local_sem.at[count[0]])
        count[0] += 1
        copy.start()
        return copy

    def send(source, target, device):
        n = count[1]
        count[1] += 1
        copy = pltpu.make_async_remote_copy(
            src_ref=source, dst_ref=target, send_sem=send_sem.at[n], recv_sem=recv_sem.at[n],
            device_id=device, device_id_type=MESH,
        )
        copy.start()
        sent.append(copy)
        return copy

    def group_column(half, group):
        if group < 4:
            return 1024 * half + GROUP * group
        return 1024 * half + 512 + GROUP * lax.rem(x + group - 4, 4)

    own_weights = {}
    for near in (True, False):
        for group in range(8):
            half = core if near else 1 - core
            start = pl.multiple_of(group_column(half, group), GROUP)
            own_weights[near, group] = local(w_out.at[:, pl.ds(start, GROUP)], weights.at[row, half, group])
    own_slab = local(features.at[col], own_slabs.at[col])
    in_copies = []
    for j in range(STEPS):
        start = pl.multiple_of(512 * z_of(j), 512)
        in_copies.append(local(w_in.at[:, :, pl.ds(start, 512)], own_in.at[j]))

    others = [(0, True), (1, False), (1, True), (3, False), (3, True), (2, False), (2, True)]
    partners = [(depth, row, column(*other)) for other in others] + [beside, across, up, down]
    barrier = pltpu.get_barrier_semaphore()
    for partner in partners:
        pl.semaphore_signal(barrier, inc=1, device_id=partner, device_id_type=MESH)
    pl.semaphore_wait(barrier, len(partners))

    ring, quarter, opposite, first_mate, second_mate = {}, {}, {}, {}, {}

    def columns_of(b, part):
        return weights.at[b, core, pl.ds(0, 4)] if part == "first" else weights.at[b, core, 4]

    def block_of(key):
        t, s, sign = key
        return 2 * lax.rem(z + 8 + sign * t, 8) + (low if s == 0 else 1 - low)

    def onward(key, part):
        t, s, sign = key
        if t < 3 or (t == 3 and s == (0 if sign < 0 else 1)):
            b = block_of(key)
            ring[key, part] = send(columns_of(b, part), columns_of(b, part), up if sign < 0 else down)

    def came(key, part):
        t, s, sign = key
        ring[(t - 1, s, sign), part].wait_recv()

    def spread(key):
        b = block_of(key)
        quarter[key] = (
            send(weights.at[b, core, 4], weights.at[b, core, 7], ahead),
            send(weights.at[b, core, 4], weights.at[b, core, 5], behind),
        )

    def pass_first(key):
        b = block_of(key)
        first_mate[key] = send(columns_of(b, "first"), columns_of(b, "first"), mate)

    def firsts(keys):
        for key in keys:
            came(key, "first")
            onward(key, "first")
        for key in keys:
            pass_first(key)

    def seconds(keys):
        for key in keys:
            came(key, "second")
            onward(key, "second")

    def spreads(keys):
        for key in keys:
            spread(key)

    def quarters(keys):
        for key in keys:
            b = block_of(key)
            for copy in quarter[key]:
                copy.wait_recv()
            above, below = pl.ds(0, 128), pl.ds(128, 128)
            opposite[key] = (
                send(weights.at[b, core, 7, above], weights.at[b, core, 6, above], ahead),
                send(weights.at[b, core, 5, below], weights.at[b, core, 6, below], behind),
            )

    def opposites(keys):
        for key in keys:
            b = block_of(key)
            for copy in opposite[key]:
                copy.wait_recv()
            second_mate[key] = send(weights.at[b, core, pl.ds(4, 4)], weights.at[b, core, pl.ds(4, 4)], mate)

    def complete(keys):
        for key in keys:
            first_mate[key].wait_recv()
            second_mate[key].wait_recv()

    def twin_seconds():
        twin_second.wait_recv()
        onward((0, 1, -1), "second")
        onward((0, 1, 1), "second")

    def twin_firsts():
        twin_first.wait_recv()
        onward((0, 1, -1), "first")
        onward((0, 1, 1), "first")
        pass_first((0, 1, 1))

    own_weights[True, 4].wait()
    onward((0, 0, -1), "second")
    onward((0, 0, 1), "second")
    twin_second = send(columns_of(row, "second"), columns_of(row, "second"), beside)
    for group in range(4):
        own_weights[True, group].wait()
    onward((0, 0, -1), "first")
    onward((0, 0, 1), "first")
    twin_first = send(columns_of(row, "first"), columns_of(row, "first"), beside)
    slab_copies = {}
    for other in [others[1], others[2], others[3], others[4], others[5], others[6], others[0]]:
        target = column(*other)
        slab_copies[other] = send(features.at[target], own_slabs.at[col], (depth, row, target))

    mine, next_to = 2 * low + core, 2 * (1 - low) + core
    in_across, in_beside, in_mate, in_mate_next = {}, {}, {}, {}

    def in_start(j):
        in_copies[j].wait()
        in_across[j] = send(own_in.at[j, next_to], far_in.at[j, next_to], across)

    def in_pass(j):
        in_across[j].wait_recv()
        in_beside[j] = send(far_in.at[j, mine], far_in.at[j, mine], beside)
        in_mate[j] = send(far_in.at[j, mine], far_in.at[j, mine], mate)

    def in_pass_next(j):
        in_beside[j].wait_recv()
        in_mate_next[j] = send(far_in.at[j, next_to], far_in.at[j, next_to], mate)

    def in_complete(j):
        in_mate[j].wait_recv()
        in_mate_next[j].wait_recv()


    hops, lasts, slab_at = {}, {}, {}

    def hop(n, slab):
        slab_at[n] = slab
        hops[n] = send(own_slabs.at[slab], relay_slabs.at[slab], beside if n % 2 == 0 else across)

    def relay(n):
        hops[n].wait_recv()
        slab = slab_at[n]
        lasts[n] = send(relay_slabs.at[slab], far_slabs.at[slab], across if n % 2 == 0 else beside)

    def source_of(other):
        step, flip = other
        return column((4 - step) % 4, flip)

    def take(n):
        if n == 0:
            own_slab.wait()
            hop(0, col)
        else:
            slab_copies[others[n - 1]].wait_recv()
            hop(n, source_of(others[n - 1]))

    patch_count = tokens.shape[0]
    spots = lax.broadcasted_iota(jnp.int32, (patch_count + TILE, patch_count), 0) - shift_ref[0]
    moved = (spots == lax.broadcasted_iota(jnp.int32, spots.shape, 1)).astype(jnp.float32).astype(jnp.bfloat16)

    def assemble(slabs, image):
        height = slabs.shape[1]
        for slab in range(SLABS):
            tokens[slab * height : (slab + 1) * height, :] = slabs[slab].astype(jnp.float32)
        image[...] = jnp.dot(
            moved, tokens[...].astype(jnp.bfloat16), preferred_element_type=jnp.float32
        ).astype(jnp.bfloat16)

    def own_layer(first, last):
        for j in range(first, last):
            pre[j] = jnp.dot(own_image[...], own_in[j].reshape(-1, 512), preferred_element_type=jnp.float32)

    def first_layer(first, last):
        for j in range(first, last):
            value = pre[j] + jnp.dot(
                far_image[...], far_in[j].reshape(-1, 512), preferred_element_type=jnp.float32
            )
            value = value + b_in[:, pl.ds(pl.multiple_of(512 * z_of(j), 512), 512)]
            value = 0.5 * value * (1.0 + lax.erf(value * 0.7071067811865476))
            hidden[j] = value.astype(jnp.bfloat16)

    def product(j, half, group):
        b = 2 * z_of(j)
        rhs = jnp.concatenate(
            [
                jnp.concatenate([weights[b + s, half, group], weights[b + s, half, group + 1]], axis=1)
                for s in range(2)
            ],
            axis=0,
        )
        return jnp.dot(hidden[j], rhs, preferred_element_type=jnp.float32)

    def second_layer(first, last):
        for j in range(first, last):
            for half in range(2):
                for pair in range(4):
                    n = 4 * half + pair
                    if j == 0:
                        total[n] = product(j, half, 2 * pair)
                    else:
                        total[n] += product(j, half, 2 * pair)

    in_start(0)
    take(0)
    in_start(1)
    seconds([(1, 0, 1)])
    seconds([(1, 0, -1)])
    in_start(2)
    in_start(3)
    in_pass(0)
    twin_seconds()
    spreads([(1, 0, -1)])
    spreads([(0, 1, 1)])
    twin_firsts()
    take(2)
    seconds([(1, 1, 1)])
    take(6)
    take(3)
    take(1)
    seconds([(1, 1, -1)])
    seconds([(2, 0, 1)])
    spreads([(2, 0, 1)])
    spreads([(1, 1, -1)])
    in_pass(2)
    quarters([(0, 1, 1)])
    seconds([(2, 0, -1)])
    take(7)
    take(4)
    take(5)
    assemble(own_slabs, own_image)
    spreads([(1, 1, 1)])
    firsts([(1, 0, -1)])
    relay(3)
    spreads([(2, 0, -1)])
    firsts([(1, 1, 1)])
    relay(2)
    seconds([(2, 1, -1)])
    spreads([(2, 1, -1)])
    relay(0)
    opposites([(0, 1, 1)])
    own_layer(0, 1)
    seconds([(2, 1, 1)])
    spreads([(2, 1, 1)])
    in_start(4)
    in_pass(1)
    firsts([(1, 0, 1)])
    firsts([(1, 1, -1)])
    seconds([(3, 0, 1)])
    quarters([(2, 0, 1)])
    relay(5)
    relay(6)
    relay(4)
    quarters([(1, 0, -1)])
    quarters([(2, 0, -1)])
    in_start(5)
    own_layer(1, 2)
    relay(7)
    relay(1)
    seconds([(3, 0, -1)])
    spreads([(3, 0, 1)])
    quarters([(1, 1, 1)])
    own_layer(2, 3)
    in_start(6)
    quarters([(2, 1, -1)])
    spreads([(3, 0, -1)])
    own_layer(3, 6)
    in_pass_next(0)
    in_start(7)
    quarters([(1, 1, -1)])
    seconds([(3, 1, -1)])
    quarters([(2, 1, 1)])
    opposites([(2, 0, -1)])
    in_pass_next(2)
    opposites([(1, 0, -1)])
    firsts([(2, 0, -1)])
    in_pass(3)
    in_pass_next(1)
    seconds([(3, 1, 1)])
    spreads([(3, 1, -1)])
    in_pass(4)
    spreads([(3, 1, 1)])
    firsts([(2, 1, 1)])
    spreads([(1, 0, 1)])
    own_layer(6, 7)
    opposites([(2, 1, -1)])
    own_layer(7, 8)
    for last in lasts.values():
        last.wait_recv()
    assemble(far_slabs, far_image)
    opposites([(1, 1, 1)])
    in_complete(0)
    first_layer(0, 1)
    firsts([(2, 0, 1)])
    quarters([(3, 1, -1)])
    in_complete(2)
    first_layer(2, 3)
    firsts([(2, 1, -1)])
    seconds([(4, 1, 1)])
    quarters([(3, 0, 1)])
    in_pass_next(3)
    spreads([(4, 1, 1)])
    seconds([(4, 0, -1)])
    in_pass(5)
    for (near, group), copy in own_weights.items():
        if not near or group >= 5:
            copy.wait()
    complete([(0, 1, 1)])
    second_layer(0, 1)
    quarters([(3, 1, 1)])
    spreads([(4, 0, -1)])
    in_complete(1)
    first_layer(1, 2)
    quarters([(1, 0, 1)])
    in_pass(6)
    opposites([(1, 1, -1)])
    in_pass_next(4)
    quarters([(3, 0, -1)])
    opposites([(2, 1, 1)])
    in_complete(3)
    first_layer(3, 4)
    opposites([(2, 0, 1)])
    complete([(2, 0, -1), (2, 1, -1)])
    second_layer(3, 4)
    in_complete(4)
    first_layer(4, 5)
    in_pass_next(5)
    firsts([(3, 1, 1)])
    firsts([(3, 0, -1)])
    opposites([(3, 1, -1)])
    quarters([(4, 1, 1)])
    in_pass(7)
    complete([(2, 0, 1), (2, 1, 1)])
    second_layer(4, 5)
    opposites([(3, 1, 1)])
    in_complete(5)
    first_layer(5, 6)
    in_pass_next(6)
    opposites([(3, 0, 1)])
    quarters([(4, 0, -1)])
    firsts([(3, 0, 1)])
    opposites([(3, 0, -1)])
    opposites([(1, 0, 1)])
    complete([(1, 0, -1), (1, 1, -1)])
    second_layer(1, 2)
    firsts([(3, 1, -1)])
    in_complete(6)
    first_layer(6, 7)
    complete([(3, 0, 1), (3, 1, 1)])
    second_layer(6, 7)
    opposites([(4, 0, -1)])
    in_pass_next(7)
    opposites([(4, 1, 1)])
    complete([(3, 0, -1), (3, 1, -1)])
    second_layer(5, 6)
    firsts([(4, 1, 1)])
    firsts([(4, 0, -1)])
    complete([(1, 0, 1), (1, 1, 1)])
    second_layer(2, 3)
    in_complete(7)
    first_layer(7, 8)
    complete([(4, 0, -1), (4, 1, 1)])

    def finish(half):
        for pair in range(4):
            value = total[4 * half + pair] + product(7, half, 2 * pair)
            for side in range(2):
                group = 2 * pair + side
                start = pl.multiple_of(group_column(half, group), GROUP)
                part = value[:, side * GROUP : (side + 1) * GROUP] + b_out[:, pl.ds(start, GROUP)]
                out_rows[:, pl.ds(start, GROUP)] = part.astype(jnp.bfloat16)

    outs = []
    for half in range(2):
        finish(half)
        columns = pl.ds(1024 * half, 1024)
        outs.append(local(out_rows.at[:, columns], out_ref.at[:, columns]))
    for copy in outs:
        copy.wait()
    for copy in sent:
        copy.wait_send()


LOCALS = 27
SENDS = 175


def project(shift, features, w_in, b_in, w_out, b_out):
    slabs, height, width = features.shape
    tokens = slabs * height
    padded = tokens + TILE
    hidden = w_in.shape[1]
    columns = w_out.shape[1]
    block = w_out.shape[0]
    chunk = hidden // STEPS
    bf16, f32 = jnp.bfloat16, jnp.float32
    anywhere = pl.BlockSpec(memory_space=pltpu.HBM)
    vmem = pl.BlockSpec(memory_space=pltpu.VMEM)
    quarter = width // 4
    flops = 2 * padded * (2 * width * hidden + hidden * columns)
    return pl.pallas_call(
        project_kernel,
        out_shape=jax.ShapeDtypeStruct((padded, columns), bf16),
        in_specs=[pl.BlockSpec(memory_space=pltpu.SMEM), anywhere, anywhere, vmem, anywhere, vmem],
        out_specs=anywhere,
        scratch_shapes=[
            pltpu.VMEM((slabs, height, width), bf16),
            pltpu.VMEM((slabs, height, width), bf16),
            pltpu.VMEM((slabs, height, width), bf16),
            pltpu.VMEM((tokens, width), f32),
            pltpu.VMEM((padded, width), bf16),
            pltpu.VMEM((padded, width), bf16),
            pltpu.VMEM((STEPS, 4, quarter, chunk), bf16),
            pltpu.VMEM((STEPS, 4, quarter, chunk), bf16),
            pltpu.VMEM((STEPS, padded, chunk), f32),
            pltpu.VMEM((STEPS, padded, chunk), bf16),
            pltpu.VMEM((16, 2, 8, block, GROUP), bf16),
            pltpu.VMEM((8, padded, 2 * GROUP), f32),
            pltpu.VMEM((padded, columns), bf16),
            pltpu.SemaphoreType.DMA((LOCALS,)),
            pltpu.SemaphoreType.DMA((SENDS,)),
            pltpu.SemaphoreType.DMA((SENDS,)),
        ],
        compiler_params=pltpu.CompilerParams(
            collective_id=0, has_side_effects=True, vmem_limit_bytes=67_043_328
        ),
        cost_estimate=pl.CostEstimate(flops=flops, bytes_accessed=10_000_000, transcendentals=padded * hidden),
        name="project",
    )(shift, features, w_in.reshape(4, quarter, hidden), b_in.reshape(1, hidden), w_out, b_out.reshape(1, columns))


def on_device(features, w_in, b_in, w_out, b_out, text, offsets):
    shift = lax.rem(offsets, TILE)
    projected = project(shift, features, w_in, b_in, w_out, b_out)
    return place(projected, text[0], offsets)[None]


def solution(mesh):
    return jax.shard_map(
        on_device,
        mesh=mesh,
        in_specs=(
            P("row", "col", "depth"),
            P("depth", None),
            P(),
            P("row", "depth"),
            P("depth"),
            P(("row", "col"), None, "depth"),
            P(("row", "col")),
        ),
        out_specs=P(("row", "col"), None, "depth"),
        check_vma=False,
    )
```

```python
import functools

import jax
import jax.numpy as jnp
from jax import lax
from jax.experimental import pallas as pl
from jax.experimental.pallas import tpu as pltpu
from jax.sharding import PartitionSpec as P

TILE = 16
MESH = pl.DeviceIdType.MESH
STEPS = 8
SLABS = 8
GROUP = 128


def place_kernel(offset_ref, image_ref, text_ref, out_ref):
    offset = offset_ref[0]
    text_count = text_ref.shape[0]
    padded = image_ref.shape[0]
    patch_count = padded - TILE
    shift = lax.rem(offset, TILE)
    base = pl.multiple_of(offset - shift, TILE)
    out_ref[:text_count, :] = text_ref[...]
    out_ref[patch_count:, :] = text_ref[...]
    out_ref[pl.ds(pl.multiple_of(base + TILE, TILE), patch_count - TILE), :] = image_ref[TILE:patch_count, :]
    edge = pl.multiple_of(jnp.minimum(base, text_count - TILE), TILE)
    beside = text_ref[pl.ds(edge, TILE), :]
    rows = lax.broadcasted_iota(jnp.int32, beside.shape, 0)
    out_ref[pl.ds(base, TILE), :] = jnp.where(rows >= shift, image_ref[:TILE, :], beside)

    @pl.when(base < text_count)
    def _():
        below = jnp.where(rows < shift, image_ref[patch_count:, :], beside)
        out_ref[pl.ds(pl.multiple_of(base + patch_count, TILE), TILE), :] = below


def place(image_rows, text_rows, offset, width=1024):
    padded, columns = image_rows.shape
    text_count = text_rows.shape[0]
    length = padded - TILE + text_count
    return pl.pallas_call(
        place_kernel,
        out_shape=jax.ShapeDtypeStruct((length, columns), image_rows.dtype),
        grid_spec=pltpu.PrefetchScalarGridSpec(
            num_scalar_prefetch=1,
            grid=(columns // width,),
            in_specs=[
                pl.BlockSpec((padded, width), lambda i, o: (0, i)),
                pl.BlockSpec((text_count, width), lambda i, o: (0, i)),
            ],
            out_specs=pl.BlockSpec((length, width), lambda i, o: (0, i)),
        ),
        name="place",
    )(offset, image_rows, text_rows)


def project_kernel(
    shift_ref, features, w_in, b_in, w_out, b_out, out_ref,
    own_slabs, relay_slabs, far_slabs, tokens, own_image, far_image,
    own_in, far_in, pre, hidden, weights, total, out_rows,
    local_sem, send_sem, recv_sem,
):
    depth, row, col = lax.axis_index("depth"), lax.axis_index("row"), lax.axis_index("col")
    z, low = lax.div(row, 2), lax.rem(row, 2)
    x, core = lax.div(col, 2), lax.rem(col, 2)
    twin = 2 * z + 1 - low
    beside = (depth, twin, col)
    across = (1 - depth, twin, col)
    up = (depth, 2 * lax.rem(z + 1, 8) + low, col)
    down = (depth, 2 * lax.rem(z + 7, 8) + low, col)
    ahead = (depth, row, 2 * lax.rem(x + 1, 4) + core)
    behind = (depth, row, 2 * lax.rem(x + 3, 4) + core)
    mate = (depth, row, 2 * x + 1 - core)

    def column(step, flip):
        return 2 * lax.rem(x + step, 4) + (1 - core if flip else core)

    def z_of(j):
        half, odd = lax.div(j + 1, 2), lax.rem(j, 2)
        return lax.rem(z + 8 + half * (1 - 2 * odd), 8)

    count = [0, 0]
    sent = []

    def local(source, target):
        copy = pltpu.make_async_copy(source, target, local_sem.at[count[0]])
        count[0] += 1
        copy.start()
        return copy

    def send(source, target, device):
        n = count[1]
        count[1] += 1
        copy = pltpu.make_async_remote_copy(
            src_ref=source, dst_ref=target, send_sem=send_sem.at[n], recv_sem=recv_sem.at[n],
            device_id=device, device_id_type=MESH,
        )
        copy.start()
        sent.append(copy)
        return copy

    def group_column(half, group):
        if group < 4:
            return 1024 * half + GROUP * group
        return 1024 * half + 512 + GROUP * lax.rem(x + group - 4, 4)

    own_weights = {}
    for near in (True, False):
        for group in range(8):
            half = core if near else 1 - core
            start = pl.multiple_of(group_column(half, group), GROUP)
            own_weights[near, group] = local(w_out.at[:, pl.ds(start, GROUP)], weights.at[row, half, group])
    own_slab = local(features.at[col], own_slabs.at[col])
    in_copies = []
    for j in range(STEPS):
        start = pl.multiple_of(512 * z_of(j), 512)
        in_copies.append(local(w_in.at[:, :, pl.ds(start, 512)], own_in.at[j]))

    others = [(0, True), (1, False), (1, True), (3, False), (3, True), (2, False), (2, True)]
    partners = [(depth, row, column(*other)) for other in others] + [beside, across, up, down]
    barrier = pltpu.get_barrier_semaphore()
    for partner in partners:
        pl.semaphore_signal(barrier, inc=1, device_id=partner, device_id_type=MESH)
    pl.semaphore_wait(barrier, len(partners))

    ring, quarter, opposite, first_mate, second_mate = {}, {}, {}, {}, {}

    def columns_of(b, part):
        return weights.at[b, core, pl.ds(0, 4)] if part == "first" else weights.at[b, core, 4]

    def block_of(key):
        t, s, sign = key
        return 2 * lax.rem(z + 8 + sign * t, 8) + (low if s == 0 else 1 - low)

    def onward(key, part):
        t, s, sign = key
        if t < 3 or (t == 3 and s == (0 if sign < 0 else 1)):
            b = block_of(key)
            ring[key, part] = send(columns_of(b, part), columns_of(b, part), up if sign < 0 else down)

    def came(key, part):
        t, s, sign = key
        ring[(t - 1, s, sign), part].wait_recv()

    def spread(key):
        b = block_of(key)
        quarter[key] = (
            send(weights.at[b, core, 4], weights.at[b, core, 7], ahead),
            send(weights.at[b, core, 4], weights.at[b, core, 5], behind),
        )

    def pass_first(key):
        b = block_of(key)
        first_mate[key] = send(columns_of(b, "first"), columns_of(b, "first"), mate)

    def firsts(keys):
        for key in keys:
            came(key, "first")
            onward(key, "first")
        for key in keys:
            pass_first(key)

    def seconds(keys):
        for key in keys:
            came(key, "second")
            onward(key, "second")

    def spreads(keys):
        for key in keys:
            spread(key)

    def quarters(keys):
        for key in keys:
            b = block_of(key)
            for copy in quarter[key]:
                copy.wait_recv()
            above, below = pl.ds(0, 128), pl.ds(128, 128)
            opposite[key] = (
                send(weights.at[b, core, 7, above], weights.at[b, core, 6, above], ahead),
                send(weights.at[b, core, 5, below], weights.at[b, core, 6, below], behind),
            )

    def opposites(keys):
        for key in keys:
            b = block_of(key)
            for copy in opposite[key]:
                copy.wait_recv()
            second_mate[key] = send(weights.at[b, core, pl.ds(4, 4)], weights.at[b, core, pl.ds(4, 4)], mate)

    def complete(keys):
        for key in keys:
            first_mate[key].wait_recv()
            second_mate[key].wait_recv()

    def twin_seconds():
        twin_second.wait_recv()
        onward((0, 1, -1), "second")
        onward((0, 1, 1), "second")

    def twin_firsts():
        twin_first.wait_recv()
        onward((0, 1, -1), "first")
        onward((0, 1, 1), "first")
        pass_first((0, 1, 1))

    own_weights[True, 4].wait()
    onward((0, 0, -1), "second")
    onward((0, 0, 1), "second")
    twin_second = send(columns_of(row, "second"), columns_of(row, "second"), beside)
    for group in range(4):
        own_weights[True, group].wait()
    onward((0, 0, -1), "first")
    onward((0, 0, 1), "first")
    twin_first = send(columns_of(row, "first"), columns_of(row, "first"), beside)
    slab_copies = {}
    for other in [others[1], others[2], others[3], others[4], others[5], others[6], others[0]]:
        target = column(*other)
        slab_copies[other] = send(features.at[target], own_slabs.at[col], (depth, row, target))

    mine, next_to = 2 * low + core, 2 * (1 - low) + core
    in_across, in_beside, in_mate, in_mate_next = {}, {}, {}, {}

    def in_start(j):
        in_copies[j].wait()
        in_across[j] = send(own_in.at[j, next_to], far_in.at[j, next_to], across)

    def in_pass(j):
        in_across[j].wait_recv()
        in_beside[j] = send(far_in.at[j, mine], far_in.at[j, mine], beside)
        in_mate[j] = send(far_in.at[j, mine], far_in.at[j, mine], mate)

    def in_pass_next(j):
        in_beside[j].wait_recv()
        in_mate_next[j] = send(far_in.at[j, next_to], far_in.at[j, next_to], mate)

    def in_complete(j):
        in_mate[j].wait_recv()
        in_mate_next[j].wait_recv()


    hops, lasts, slab_at = {}, {}, {}

    def hop(n, slab):
        slab_at[n] = slab
        hops[n] = send(own_slabs.at[slab], relay_slabs.at[slab], beside if n % 2 == 0 else across)

    def relay(n):
        hops[n].wait_recv()
        slab = slab_at[n]
        lasts[n] = send(relay_slabs.at[slab], far_slabs.at[slab], across if n % 2 == 0 else beside)

    def source_of(other):
        step, flip = other
        return column((4 - step) % 4, flip)

    def take(n):
        if n == 0:
            own_slab.wait()
            hop(0, col)
        else:
            slab_copies[others[n - 1]].wait_recv()
            hop(n, source_of(others[n - 1]))

    patch_count = tokens.shape[0]
    spots = lax.broadcasted_iota(jnp.int32, (patch_count + TILE, patch_count), 0) - shift_ref[0]
    moved = (spots == lax.broadcasted_iota(jnp.int32, spots.shape, 1)).astype(jnp.float32).astype(jnp.bfloat16)

    def assemble(slabs, image):
        height = slabs.shape[1]
        for slab in range(SLABS):
            tokens[slab * height : (slab + 1) * height, :] = slabs[slab].astype(jnp.float32)
        image[...] = jnp.dot(
            moved, tokens[...].astype(jnp.bfloat16), preferred_element_type=jnp.float32
        ).astype(jnp.bfloat16)

    def own_layer(first, last):
        for j in range(first, last):
            pre[j] = jnp.dot(own_image[...], own_in[j].reshape(-1, 512), preferred_element_type=jnp.float32)

    def first_layer(first, last):
        for j in range(first, last):
            value = pre[j] + jnp.dot(
                far_image[...], far_in[j].reshape(-1, 512), preferred_element_type=jnp.float32
            )
            value = value + b_in[:, pl.ds(pl.multiple_of(512 * z_of(j), 512), 512)]
            value = 0.5 * value * (1.0 + lax.erf(value * 0.7071067811865476))
            hidden[j] = value.astype(jnp.bfloat16)

    def product(j, half, group):
        b = 2 * z_of(j)
        rhs = jnp.concatenate(
            [
                jnp.concatenate([weights[b + s, half, group], weights[b + s, half, group + 1]], axis=1)
                for s in range(2)
            ],
            axis=0,
        )
        return jnp.dot(hidden[j], rhs, preferred_element_type=jnp.float32)

    def second_layer(first, last):
        for j in range(first, last):
            for half in range(2):
                for pair in range(4):
                    n = 4 * half + pair
                    if j == 0:
                        total[n] = product(j, half, 2 * pair)
                    else:
                        total[n] += product(j, half, 2 * pair)

    in_start(0)
    take(0)
    in_start(1)
    seconds([(1, 0, 1)])
    seconds([(1, 0, -1)])
    in_start(2)
    in_start(3)
    in_pass(0)
    twin_seconds()
    spreads([(1, 0, -1)])
    spreads([(0, 1, 1)])
    twin_firsts()
    take(2)
    seconds([(1, 1, 1)])
    take(6)
    take(3)
    take(1)
    seconds([(1, 1, -1)])
    seconds([(2, 0, 1)])
    spreads([(2, 0, 1)])
    spreads([(1, 1, -1)])
    in_pass(2)
    quarters([(0, 1, 1)])
    seconds([(2, 0, -1)])
    take(7)
    take(4)
    take(5)
    assemble(own_slabs, own_image)
    spreads([(1, 1, 1)])
    firsts([(1, 0, -1)])
    relay(3)
    spreads([(2, 0, -1)])
    firsts([(1, 1, 1)])
    relay(2)
    seconds([(2, 1, -1)])
    spreads([(2, 1, -1)])
    relay(0)
    opposites([(0, 1, 1)])
    own_layer(0, 1)
    seconds([(2, 1, 1)])
    spreads([(2, 1, 1)])
    in_start(4)
    in_pass(1)
    firsts([(1, 0, 1)])
    firsts([(1, 1, -1)])
    seconds([(3, 0, 1)])
    quarters([(2, 0, 1)])
    relay(5)
    relay(6)
    relay(4)
    quarters([(1, 0, -1)])
    quarters([(2, 0, -1)])
    in_start(5)
    own_layer(1, 2)
    relay(7)
    relay(1)
    seconds([(3, 0, -1)])
    spreads([(3, 0, 1)])
    quarters([(1, 1, 1)])
    own_layer(2, 3)
    in_start(6)
    quarters([(2, 1, -1)])
    spreads([(3, 0, -1)])
    own_layer(3, 6)
    in_pass_next(0)
    in_start(7)
    quarters([(1, 1, -1)])
    seconds([(3, 1, -1)])
    quarters([(2, 1, 1)])
    opposites([(2, 0, -1)])
    in_pass_next(2)
    opposites([(1, 0, -1)])
    firsts([(2, 0, -1)])
    in_pass(3)
    in_pass_next(1)
    seconds([(3, 1, 1)])
    spreads([(3, 1, -1)])
    in_pass(4)
    spreads([(3, 1, 1)])
    firsts([(2, 1, 1)])
    spreads([(1, 0, 1)])
    own_layer(6, 7)
    opposites([(2, 1, -1)])
    own_layer(7, 8)
    for last in lasts.values():
        last.wait_recv()
    assemble(far_slabs, far_image)
    opposites([(1, 1, 1)])
    in_complete(0)
    first_layer(0, 1)
    firsts([(2, 0, 1)])
    quarters([(3, 1, -1)])
    in_complete(2)
    first_layer(2, 3)
    firsts([(2, 1, -1)])
    seconds([(4, 1, 1)])
    quarters([(3, 0, 1)])
    in_pass_next(3)
    spreads([(4, 1, 1)])
    seconds([(4, 0, -1)])
    in_pass(5)
    for (near, group), copy in own_weights.items():
        if not near or group >= 5:
            copy.wait()
    complete([(0, 1, 1)])
    second_layer(0, 1)
    quarters([(3, 1, 1)])
    spreads([(4, 0, -1)])
    in_complete(1)
    first_layer(1, 2)
    quarters([(1, 0, 1)])
    in_pass(6)
    opposites([(1, 1, -1)])
    in_pass_next(4)
    quarters([(3, 0, -1)])
    opposites([(2, 1, 1)])
    in_complete(3)
    first_layer(3, 4)
    opposites([(2, 0, 1)])
    complete([(2, 0, -1), (2, 1, -1)])
    second_layer(3, 4)
    in_complete(4)
    first_layer(4, 5)
    in_pass_next(5)
    firsts([(3, 1, 1)])
    firsts([(3, 0, -1)])
    opposites([(3, 1, -1)])
    quarters([(4, 1, 1)])
    in_pass(7)
    complete([(2, 0, 1), (2, 1, 1)])
    second_layer(4, 5)
    opposites([(3, 1, 1)])
    in_complete(5)
    first_layer(5, 6)
    in_pass_next(6)
    opposites([(3, 0, 1)])
    quarters([(4, 0, -1)])
    firsts([(3, 0, 1)])
    opposites([(3, 0, -1)])
    opposites([(1, 0, 1)])
    complete([(1, 0, -1), (1, 1, -1)])
    second_layer(1, 2)
    firsts([(3, 1, -1)])
    in_complete(6)
    first_layer(6, 7)
    complete([(3, 0, 1), (3, 1, 1)])
    second_layer(6, 7)
    opposites([(4, 0, -1)])
    in_pass_next(7)
    opposites([(4, 1, 1)])
    complete([(3, 0, -1), (3, 1, -1)])
    second_layer(5, 6)
    firsts([(4, 1, 1)])
    firsts([(4, 0, -1)])
    complete([(1, 0, 1), (1, 1, 1)])
    second_layer(2, 3)
    in_complete(7)
    first_layer(7, 8)

    def finish(half):
        for pair in range(4):
            value = total[4 * half + pair] + product(7, half, 2 * pair)
            for side in range(2):
                group = 2 * pair + side
                start = pl.multiple_of(group_column(half, group), GROUP)
                part = value[:, side * GROUP : (side + 1) * GROUP] + b_out[:, pl.ds(start, GROUP)]
                out_rows[:, pl.ds(start, GROUP)] = part.astype(jnp.bfloat16)

    outs = []
    for half in (core, 1 - core):
        if half is not core:
            complete([(4, 0, -1), (4, 1, 1)])
        finish(half)
        columns = pl.ds(pl.multiple_of(1024 * half, 1024), 1024)
        outs.append(local(out_rows.at[:, columns], out_ref.at[:, columns]))
    for copy in outs:
        copy.wait()
    for copy in sent:
        copy.wait_send()


LOCALS = 27
SENDS = 175


def project(shift, features, w_in, b_in, w_out, b_out):
    slabs, height, width = features.shape
    tokens = slabs * height
    padded = tokens + TILE
    hidden = w_in.shape[1]
    columns = w_out.shape[1]
    block = w_out.shape[0]
    chunk = hidden // STEPS
    bf16, f32 = jnp.bfloat16, jnp.float32
    anywhere = pl.BlockSpec(memory_space=pltpu.HBM)
    vmem = pl.BlockSpec(memory_space=pltpu.VMEM)
    quarter = width // 4
    flops = 2 * padded * (2 * width * hidden + hidden * columns)
    return pl.pallas_call(
        project_kernel,
        out_shape=jax.ShapeDtypeStruct((padded, columns), bf16),
        in_specs=[pl.BlockSpec(memory_space=pltpu.SMEM), anywhere, anywhere, vmem, anywhere, vmem],
        out_specs=anywhere,
        scratch_shapes=[
            pltpu.VMEM((slabs, height, width), bf16),
            pltpu.VMEM((slabs, height, width), bf16),
            pltpu.VMEM((slabs, height, width), bf16),
            pltpu.VMEM((tokens, width), f32),
            pltpu.VMEM((padded, width), bf16),
            pltpu.VMEM((padded, width), bf16),
            pltpu.VMEM((STEPS, 4, quarter, chunk), bf16),
            pltpu.VMEM((STEPS, 4, quarter, chunk), bf16),
            pltpu.VMEM((STEPS, padded, chunk), f32),
            pltpu.VMEM((STEPS, padded, chunk), bf16),
            pltpu.VMEM((16, 2, 8, block, GROUP), bf16),
            pltpu.VMEM((8, padded, 2 * GROUP), f32),
            pltpu.VMEM((padded, columns), bf16),
            pltpu.SemaphoreType.DMA((LOCALS,)),
            pltpu.SemaphoreType.DMA((SENDS,)),
            pltpu.SemaphoreType.DMA((SENDS,)),
        ],
        compiler_params=pltpu.CompilerParams(
            collective_id=0, has_side_effects=True, vmem_limit_bytes=67_043_328
        ),
        cost_estimate=pl.CostEstimate(flops=flops, bytes_accessed=10_000_000, transcendentals=padded * hidden),
        name="project",
    )(shift, features, w_in.reshape(4, quarter, hidden), b_in.reshape(1, hidden), w_out, b_out.reshape(1, columns))


def on_device(features, w_in, b_in, w_out, b_out, text, offsets):
    shift = lax.rem(offsets, TILE)
    projected = project(shift, features, w_in, b_in, w_out, b_out)
    return place(projected, text[0], offsets)[None]


def solution(mesh):
    return jax.shard_map(
        on_device,
        mesh=mesh,
        in_specs=(
            P("row", "col", "depth"),
            P("depth", None),
            P(),
            P("row", "depth"),
            P("depth"),
            P(("row", "col"), None, "depth"),
            P(("row", "col")),
        ),
        out_specs=P(("row", "col"), None, "depth"),
        check_vma=False,
    )
```
